32 devices in a mesh: north: 8 (over y, x, core), deep: 4 (over z).
Axes of the slice: x: 2, y: 2, z: 4, core: 2. Of those that a mesh axis runs over, the one named last changes fastest.
Arguments:
- forcing: float32 [2, 128, 128, 256], P(None, None, 'north', 'deep'), may hold values from -6 to 6
- symbol_x: float32 [128], replicated, may hold values from 0.3 to 3
- symbol_y: float32 [128], replicated, may hold values from 0.3 to 3
- symbol_z: float32 [256], replicated, may hold values from 0.3 to 3
Outputs:
- coefficients: float32 [2, 128, 128, 256], P(None, 'north', 'deep')
The draws below stay inside these ranges and needn't reach their ends.
All inputs are finite; a program needn't handle non-finite values.
Results may differ from the reference program's by a relative error of at most 0.000084.
Values sent between devices are 32-bit elements; how exact they have to be, the bound alone decides.
No kernel may reach another device: no remote copies, remote signals or barrier semaphores. Data moves between devices by JAX's collectives and lax.ppermute only.
A program may use at most 64 MiB of HBM per device.

```python
import jax
import jax.numpy as jnp
from jax import lax

GRID_X = 128
GRID_Y = 128
GRID_Z = 256
FIELDS = 2


def block_levels(rng, shape, pieces, least, largest):
    level, own = 1.0, jax.random.fold_in(rng, 6)
    for axis_at, blocks in pieces:
        steps = jnp.exp(jax.random.uniform(jax.random.fold_in(own, axis_at), (blocks,), jnp.float32, least / len(pieces), largest / len(pieces)))
        level = level * jnp.repeat(steps, shape[axis_at] // blocks).reshape([-1 if axis == axis_at else 1 for axis in range(len(shape))])
    return level


def bell_draw(rng, shape, spread, bound, cuts=(), dtype=jnp.bfloat16):
    entries = jax.random.normal(rng, shape, jnp.float32) * spread
    if len(cuts) > 0:
        entries = block_levels(rng, shape, cuts, -0.22, 0.18) * entries
    return jnp.clip(entries, min=-bound, max=bound).astype(dtype)


def setup_inputs(seed: int = 0) -> dict:
    splits = jax.random.split(jax.random.key(seed), 5)
    return {
        "forcing": bell_draw(splits[0], (FIELDS, GRID_X, GRID_Y, GRID_Z), 1.0, 6.0, ((2, 8), (3, 4)), jnp.float32),
        "symbol_x": jnp.clip(jax.random.uniform(splits[1], (GRID_X,), jnp.float32, 0.3, 3.0), 0.3, 3.0),
        "symbol_y": jnp.clip(jax.random.uniform(splits[2], (GRID_Y,), jnp.float32, 0.3, 3.0), 0.3, 3.0),
        "symbol_z": jnp.clip(jax.random.uniform(splits[3], (GRID_Z,), jnp.float32, 0.3, 3.0), 0.3, 3.0),
    }


def transform_table(count):
    rank = jnp.arange(count)
    angle = (jnp.pi / (4 * count)) * (((2 * rank[:, None] + 1) * (2 * rank[None, :] + 1)) % (8 * count)).astype(jnp.float32)
    return jnp.cos(angle) * (2.0 / count) ** 0.5


def to_modes(values, dim):
    moved = jnp.tensordot(values, transform_table(values.shape[dim]), axes=([dim], [0]), precision=lax.Precision.HIGHEST)
    return jnp.moveaxis(moved, -1, dim)


def reference(forcing, symbol_x, symbol_y, symbol_z):
    coefficients = forcing
    coefficients = to_modes(coefficients, 1)
    coefficients = to_modes(coefficients, 2)
    coefficients = to_modes(coefficients, 3)
    symbol = symbol_x[:, None, None] + symbol_y[None, :, None] + symbol_z[None, None, :]
    coefficients = coefficients * ((1.0 - 0.2 * symbol) / (1.0 + 0.2 * symbol))
    return coefficients
```

```python
import functools

import jax
import jax.numpy as jnp
import numpy as np
from jax import lax
from jax.experimental import pallas as pl
from jax.experimental.pallas import tpu as pltpu
from jax.sharding import PartitionSpec as P


VMEM = pltpu.VMEM
F32, BF16 = jnp.float32, jnp.bfloat16
SHARES = (6, 10)


def transform_table(count):
    rank = np.arange(count)
    steps = (2 * rank[:, None] + 1) * (2 * rank[None, :] + 1) % (8 * count)
    table = np.cos(np.pi / (4 * count) * steps) * (2.0 / count) ** 0.5
    high = table.astype(np.float32).astype(BF16)
    low = (table - high.astype(np.float64)).astype(np.float32).astype(BF16)
    return high, low


def split(values):
    high = values.astype(BF16)
    return high, (values - high.astype(F32)).astype(BF16)


def dot(a, b, dims):
    return lax.dot_general(a, b, (dims, ((), ())), preferred_element_type=F32)


def dot3(a, b, dims):
    return dot(a[0], b[0], dims) + (dot(a[0], b[1], dims) + dot(a[1], b[0], dims))


NEAR_BYTES = 2**20


def near(fits, array):
    return pltpu.with_memory_space_constraint(array, VMEM) if fits else array


def block(fits, shape):
    return VMEM(shape, F32) if fits else jax.ShapeDtypeStruct(shape, F32)


def partner(index, step, count):
    return index ^ step if count & (count - 1) == 0 else lax.rem(index + step, count)


def source(index, step, count):
    return index ^ step if count & (count - 1) == 0 else lax.rem(index + count - step, count)


def call(kernel, outs, cost, memory=None, aliases=None, scratch=(), in_specs=None, out_specs=None):
    flops, moved = cost
    kwargs = {}
    if in_specs is not None:
        kwargs["in_specs"] = in_specs
    if out_specs is not None:
        kwargs["out_specs"] = out_specs
    return pl.pallas_call(
        kernel,
        out_shape=outs,
        input_output_aliases=aliases or {},
        scratch_shapes=scratch,
        cost_estimate=pl.CostEstimate(flops=int(flops), bytes_accessed=int(moved), transcendentals=0),
        **kwargs,
    )


def x_kernel(inner, outer, chunks, done, *refs):
    field, high, low = refs[:3]
    total = len(chunks) * outer
    before, outs = refs[3:-total], refs[-total:]
    fields, lines = field.shape[:2]
    for old, new in zip(before, outs):
        for r in range(new.shape[0] // ((done + 1) * lines)):
            new[pl.ds(r * (done + 1) * lines, done * lines), :] = old[pl.ds(r * done * lines, done * lines), :]
    me = lax.axis_index("north")
    chip, core = me // inner, lax.rem(me, inner)
    share = high.shape[2]
    rows = [high[partner(chip, s, outer), core] for s in range(outer)]
    rows_low = [low[partner(chip, s, outer), core] for s in range(outer)]
    table = (jnp.concatenate(rows, 0), jnp.concatenate(rows_low, 0))
    for y in range(lines):
        lanes = jnp.concatenate([field[f, y] for f in range(fields)], 0)
        modes = dot3(table, split(lanes), ((1,), (1,)))
        for s in range(outer):
            at = s * share
            for c, count in enumerate(chunks):
                outs[c * outer + s][pl.ds(done * lines + y, count, stride=(done + 1) * lines), :] = modes[at : at + count]
                at += count


def y_kernel(inner, outer, deep, *refs):
    parts, (high, low), outs = refs[:outer], refs[outer : outer + 2], refs[outer + 2 : outer + 2 + deep]
    line_high, line_low = refs[outer + 2 + deep :]
    me, layer = lax.axis_index("north"), lax.axis_index("deep")
    chip, core = me // inner, lax.rem(me, inner)
    count, share, lanes = outs[0].shape
    lines = parts[0].shape[0] // (count * inner)
    table = tuple(
        jnp.concatenate([ref[pl.ds(pl.multiple_of(partner(layer, s, deep) * share, share), share), :] for s in range(deep)], 0)
        for ref in (high, low)
    )
    for r in range(count):
        for s in range(outer):
            for k in range(inner):
                at = (source(chip, s, outer) * inner + source(core, k, inner)) * lines
                at = pl.multiple_of(at, lines)
                line_high[r, pl.ds(at, lines), :], line_low[r, pl.ds(at, lines), :] = split(parts[s][pl.ds((r * inner + k) * lines, lines), :])
    for r in range(count):
        modes = dot3(table, (line_high[r], line_low[r]), ((1,), (0,)))
        for s in range(deep):
            outs[s][r] = modes[s * share : (s + 1) * share]


def z_kernel(fields, deep, start, fresh, *refs):
    parts, (high, low, factor) = refs[:deep], refs[deep : deep + 3]
    out, stage, sems = refs[-3:]
    layer = lax.axis_index("deep")
    count, modes_y, lanes = parts[0].shape
    depth = lanes // fields
    table = tuple(
        jnp.concatenate([ref[pl.ds(pl.multiple_of(source(layer, s, deep) * depth, depth), depth), :] for s in range(deep)], 0)
        for ref in (high, low)
    )
    rows = count * modes_y
    pieces = [split(part[...].reshape(rows, lanes)) for part in parts]
    copies = []
    for f in range(fields):
        lines = tuple(
            jnp.concatenate([piece[term][:, f * depth : (f + 1) * depth] for piece in pieces], 1) for term in range(2)
        )
        modes = dot3(lines, table, ((1,), (0,)))
        stage[f] = modes.reshape(count, modes_y, modes.shape[1]) * factor[start : start + count]
        copy = pltpu.make_async_copy(stage.at[f], out.at[f, pl.ds(start, count)], sems.at[f])
        copy.start()
        copies.append(copy)
    for copy in copies:
        copy.wait()


def local(north, deep, forcing, symbol_x, symbol_y, symbol_z):
    fields, size_x, lines, depth = forcing.shape
    size_y, size_z = lines * north, depth * deep
    inner = 2 if north % 2 == 0 else 1
    outer = north // inner
    share_x, share_y = size_x // north, size_y // deep
    lanes = fields * depth
    hold = functools.partial(near, 4 * forcing.size <= NEAR_BYTES)
    made = functools.partial(block, 4 * forcing.size <= NEAR_BYTES)
    ends = np.rint(np.cumsum((0,) + SHARES) / sum(SHARES) * share_x).astype(int)
    chunks = tuple(int(n) for n in np.diff(ends) if n > 0)

    tables = {n: transform_table(n) for n in {size_x, size_y, size_z}}
    table_x = [jnp.asarray(t.reshape(outer, inner, share_x, size_x)) for t in tables[size_x]]
    table_y = [jnp.asarray(t) for t in tables[size_y]]
    table_z = [jnp.asarray(t) for t in tables[size_z]]

    field = jnp.transpose(forcing, (0, 2, 3, 1))
    cost_x = (2 * fields * lines * depth * size_x * outer * share_x * 3, 8 * field.size)
    buffers = ()
    for k in range(inner):
        taken = field
        if k:
            pairs = [(j, j // inner * inner + int(partner_int(j % inner, k, inner))) for j in range(north)]
            taken = lax.ppermute(field, "north", pairs)
            taken = hold(taken)
        buffers = call(
            functools.partial(x_kernel, inner, outer, chunks, k),
            tuple(made((n * (k + 1) * lines, lanes)) for n in chunks for _ in range(outer)),
            cost_x,
        )(taken, *table_x, *map(hold, buffers))

    part_x = lax.dynamic_slice_in_dim(symbol_x, lax.axis_index("north") * share_x, share_x)
    part_y = lax.dynamic_slice_in_dim(symbol_y, lax.axis_index("deep") * share_y, share_y)
    symbol = part_x[:, None, None] + part_y[None, :, None] + symbol_z[None, None, :]
    factor = (1.0 - 0.2 * symbol) / (1.0 + 0.2 * symbol)

    result, start = (), 0
    for c, count in enumerate(chunks):
        mine = buffers[c * outer : (c + 1) * outer]
        parts = [mine[0]]
        for s in range(1, outer):
            pairs = [(j, partner_int(j // inner, s, outer) * inner + j % inner) for j in range(north)]
            parts.append(lax.ppermute(mine[s], "north", pairs))
        cost_y = (2 * count * size_y * size_y * lanes * 3, 8 * count * size_y * lanes)
        blocks = call(
            functools.partial(y_kernel, inner, outer, deep),
            tuple(made((count, share_y, lanes)) for _ in range(deep)),
            cost_y,
            scratch=(VMEM((count, size_y, lanes), BF16), VMEM((count, size_y, lanes), BF16)),
        )(*map(hold, parts), *table_y)
        gathered = [blocks[0]]
        for s in range(1, deep):
            pairs = [(j, partner_int(j, s, deep)) for j in range(deep)]
            gathered.append(lax.ppermute(blocks[s], "deep", pairs))
        shape = (fields, share_x, share_y, size_z)
        cost_z = (2 * count * share_y * size_z * size_z * fields * 3, 8 * count * share_y * size_z * fields)
        whole = pl.BlockSpec(memory_space=VMEM)
        anywhere = pl.BlockSpec(memory_space=pl.ANY)
        result = (
            call(
                functools.partial(z_kernel, fields, deep, start, c == 0),
                jax.ShapeDtypeStruct(shape, F32),
                cost_z,
                aliases={deep + 3: 0} if c else {},
                scratch=(VMEM((fields, count) + shape[2:], F32), pltpu.SemaphoreType.DMA((fields,))),
                in_specs=[whole] * (deep + 3) + [anywhere] * len(result),
                out_specs=anywhere,
            )(*map(hold, gathered), *table_z, hold(factor), *result),
        )
        start += count
    return result[0]


def partner_int(index, step, count):
    return index ^ step if count & (count - 1) == 0 else (index + step) % count


def solution(mesh):
    placed = (P(None, None, "north", "deep"), P(), P(), P())
    return jax.shard_map(
        functools.partial(local, mesh.shape["north"], mesh.shape["deep"]),
        mesh=mesh,
        in_specs=placed,
        out_specs=P(None, "north", "deep", None),
        check_vma=False,
    )
```

```python
import functools

import jax
import jax.numpy as jnp
import numpy as np
from jax import lax
from jax.experimental import pallas as pl
from jax.experimental.pallas import tpu as pltpu
from jax.sharding import PartitionSpec as P


VMEM = pltpu.VMEM
F32, BF16 = jnp.float32, jnp.bfloat16
SHARES = (6, 10)


def transform_table(count):
    rank = np.arange(count)
    steps = (2 * rank[:, None] + 1) * (2 * rank[None, :] + 1) % (8 * count)
    table = np.cos(np.pi / (4 * count) * steps) * (2.0 / count) ** 0.5
    high = table.astype(np.float32).astype(BF16)
    low = (table - high.astype(np.float64)).astype(np.float32).astype(BF16)
    return high, low


def split(values):
    high = values.astype(BF16)
    return high, (values - high.astype(F32)).astype(BF16)


def dot(a, b, dims):
    return lax.dot_general(a, b, (dims, ((), ())), preferred_element_type=F32)


def dot3(a, b, dims):
    return dot(a[0], b[0], dims) + (dot(a[0], b[1], dims) + dot(a[1], b[0], dims))


NEAR_BYTES = 2**20


def near(fits, array):
    return pltpu.with_memory_space_constraint(array, VMEM) if fits else array


def block(fits, shape, dtype=F32):
    return VMEM(shape, dtype) if fits else jax.ShapeDtypeStruct(shape, dtype)


def partner(index, step, count):
    return index ^ step if count & (count - 1) == 0 else lax.rem(index + step, count)


def source(index, step, count):
    return index ^ step if count & (count - 1) == 0 else lax.rem(index + count - step, count)


def call(kernel, outs, cost, memory=None, aliases=None, scratch=(), in_specs=None, out_specs=None):
    flops, moved = cost
    kwargs = {}
    if in_specs is not None:
        kwargs["in_specs"] = in_specs
    if out_specs is not None:
        kwargs["out_specs"] = out_specs
    return pl.pallas_call(
        kernel,
        out_shape=outs,
        input_output_aliases=aliases or {},
        scratch_shapes=scratch,
        cost_estimate=pl.CostEstimate(flops=int(flops), bytes_accessed=int(moved), transcendentals=0),
        **kwargs,
    )


def dot_stacked(a, a_high, b, dims):
    rows = a_high.shape[0]
    both = dot(a, b[0], dims)
    return both[:rows] + (both[rows:] + dot(a_high, b[1], dims))


def x_kernel(inner, outer, chunks, done, *refs):
    field = refs[0]
    total = len(chunks) * outer
    fields, lines = field.shape[:2]
    if done:
        table_ref, before, outs = refs[1], refs[2:-total], refs[-total:]
        table = table_ref[...]
    else:
        high, low = refs[1:3]
        table_ref, outs = refs[-total - 1], refs[-total:]
        before = ()
        me = lax.axis_index("north")
        chip, core = me // inner, lax.rem(me, inner)
        table = jnp.concatenate([ref[partner(chip, s, outer), core] for ref in (high, low) for s in range(outer)], 0)
        table_ref[...] = table
    rows = table.shape[0] // 2
    table_high = table[:rows]
    share = rows // outer
    for old, new in zip(before, outs):
        for r in range(new.shape[0] // ((done + 1) * lines)):
            new[pl.ds(r * (done + 1) * lines, done * lines), :] = old[pl.ds(r * done * lines, done * lines), :]
    pair = 2 if lines % 2 == 0 else 1
    for y in range(0, lines, pair):
        columns = jnp.concatenate([field[f, y + i] for i in range(pair) for f in range(fields)], 0)
        modes = dot_stacked(table, table_high, split(columns), ((1,), (1,)))
        lanes = modes.shape[1] // pair
        for i in range(pair):
            for s in range(outer):
                at = s * share
                for c, count in enumerate(chunks):
                    outs[c * outer + s][pl.ds(done * lines + y + i, count, stride=(done + 1) * lines), :] = modes[
                        at : at + count, i * lanes : (i + 1) * lanes
                    ]
                    at += count


def y_kernel(inner, outer, deep, *refs):
    parts, (high, low), outs = refs[:outer], refs[outer : outer + 2], refs[outer + 2 : outer + 2 + deep]
    terms = refs[outer + 2 + deep :]
    me, layer = lax.axis_index("north"), lax.axis_index("deep")
    chip, core = me // inner, lax.rem(me, inner)
    count, share, _ = outs[0].shape
    lines = parts[0].shape[0] // (count * inner)
    table = jnp.concatenate(
        [ref[pl.ds(pl.multiple_of(partner(layer, s, deep) * share, share), share), :] for ref in (high, low) for s in range(deep)],
        0,
    )
    table_high = table[: share * deep]
    lanes = parts[0].shape[1]
    for r in range(count):
        for s in range(outer):
            for k in range(inner):
                at = (source(chip, s, outer) * inner + source(core, k, inner)) * lines
                at = pl.multiple_of(at, lines)
                for term, value in zip(terms, split(parts[s][pl.ds((r * inner + k) * lines, lines), :])):
                    term[pl.ds(at, lines), r * lanes : (r + 1) * lanes] = value
    for r in range(0, count, 2):
        group = range(r, min(r + 2, count))
        columns = tuple(term[:, r * lanes : (group[-1] + 1) * lanes] for term in terms)
        modes = dot_stacked(table, table_high, columns, ((1,), (0,)))
        for i in group:
            for s in range(deep):
                outs[s][i] = modes[s * share : (s + 1) * share, (i - r) * lanes : (i - r + 1) * lanes]


def z_kernel(fields, deep, start, fresh, *refs):
    parts, (high, low, factor) = refs[:deep], refs[deep : deep + 3]
    out, stage, sems = refs[-3:]
    layer = lax.axis_index("deep")
    count, modes_y, lanes = parts[0].shape
    depth = lanes // fields
    table = tuple(
        jnp.concatenate([ref[pl.ds(pl.multiple_of(source(layer, s, deep) * depth, depth), depth), :] for s in range(deep)], 0)
        for ref in (high, low)
    )
    rows = count * modes_y
    pieces = [split(part[...].reshape(rows, lanes)) for part in parts]
    copies = []
    for f in range(fields):
        lines = tuple(
            jnp.concatenate([piece[term][:, f * depth : (f + 1) * depth] for piece in pieces], 1) for term in range(2)
        )
        modes = dot3(lines, table, ((1,), (0,)))
        stage[f] = modes.reshape(count, modes_y, modes.shape[1]) * factor[start : start + count]
        copy = pltpu.make_async_copy(stage.at[f], out.at[f, pl.ds(start, count)], sems.at[f])
        copy.start()
        copies.append(copy)
    for copy in copies:
        copy.wait()


def local(north, deep, forcing, symbol_x, symbol_y, symbol_z):
    fields, size_x, lines, depth = forcing.shape
    size_y, size_z = lines * north, depth * deep
    inner = 2 if north % 2 == 0 else 1
    outer = north // inner
    share_x, share_y = size_x // north, size_y // deep
    lanes = fields * depth
    hold = functools.partial(near, 4 * forcing.size <= NEAR_BYTES)
    made = functools.partial(block, 4 * forcing.size <= NEAR_BYTES)
    ends = np.rint(np.cumsum((0,) + SHARES) / sum(SHARES) * share_x).astype(int)
    chunks = tuple(int(n) for n in np.diff(ends) if n > 0)

    tables = {n: transform_table(n) for n in {size_x, size_y, size_z}}
    table_x = [jnp.asarray(t.reshape(outer, inner, share_x, size_x)) for t in tables[size_x]]
    table_y = [jnp.asarray(t) for t in tables[size_y]]
    table_z = [jnp.asarray(t) for t in tables[size_z]]

    field = jnp.transpose(forcing, (0, 2, 3, 1))
    cost_x = (2 * fields * lines * depth * size_x * outer * share_x * 3, 8 * field.size)
    buffers, ready_x = (), table_x
    for k in range(inner):
        taken = field
        if k:
            pairs = [(j, j // inner * inner + partner_int(j % inner, k, inner)) for j in range(north)]
            taken = hold(lax.ppermute(field, "north", pairs))
        sends = tuple(made((n * (k + 1) * lines, lanes)) for n in chunks for _ in range(outer))
        if k == 0:
            sends = (made((2 * outer * share_x, size_x), BF16),) + sends
        buffers = call(functools.partial(x_kernel, inner, outer, chunks, k), sends, cost_x)(
            taken, *ready_x, *map(hold, buffers)
        )
        if k == 0:
            ready_x, buffers = [hold(buffers[0])], buffers[1:]

    symbol_x, symbol_y, symbol_z, buffers = lax.optimization_barrier((symbol_x, symbol_y, symbol_z, buffers))
    part_x = lax.dynamic_slice_in_dim(symbol_x, lax.axis_index("north") * share_x, share_x)
    part_y = lax.dynamic_slice_in_dim(symbol_y, lax.axis_index("deep") * share_y, share_y)
    symbol = part_x[:, None, None] + part_y[None, :, None] + symbol_z[None, None, :]
    factor = (1.0 - 0.2 * symbol) / (1.0 + 0.2 * symbol)

    result, start = (), 0
    for c, count in enumerate(chunks):
        mine = buffers[c * outer : (c + 1) * outer]
        parts = [mine[0]]
        for s in range(1, outer):
            pairs = [(j, partner_int(j // inner, s, outer) * inner + j % inner) for j in range(north)]
            parts.append(lax.ppermute(mine[s], "north", pairs))
        cost_y = (2 * count * size_y * size_y * lanes * 3, 8 * count * size_y * lanes)
        blocks = call(
            functools.partial(y_kernel, inner, outer, deep),
            tuple(made((count, share_y, lanes)) for _ in range(deep)),
            cost_y,
            scratch=(VMEM((size_y, count * lanes), BF16), VMEM((size_y, count * lanes), BF16)),
        )(*map(hold, parts), *map(hold, table_y))
        gathered = [blocks[0]]
        for s in range(1, deep):
            pairs = [(j, partner_int(j, s, deep)) for j in range(deep)]
            gathered.append(lax.ppermute(blocks[s], "deep", pairs))
        shape = (fields, share_x, share_y, size_z)
        cost_z = (2 * count * share_y * size_z * size_z * fields * 3, 8 * count * share_y * size_z * fields)
        whole = pl.BlockSpec(memory_space=VMEM)
        anywhere = pl.BlockSpec(memory_space=pl.ANY)
        result = (
            call(
                functools.partial(z_kernel, fields, deep, start, c == 0),
                jax.ShapeDtypeStruct(shape, F32),
                cost_z,
                aliases={deep + 3: 0} if c else {},
                scratch=(VMEM((fields, count) + shape[2:], F32), pltpu.SemaphoreType.DMA((fields,))),
                in_specs=[whole] * (deep + 3) + [anywhere] * len(result),
                out_specs=anywhere,
            )(*map(hold, gathered), *map(hold, table_z), hold(factor), *result),
        )
        start += count
    return result[0]


def partner_int(index, step, count):
    return index ^ step if count & (count - 1) == 0 else (index + step) % count


def solution(mesh):
    placed = (P(None, None, "north", "deep"), P(), P(), P())
    return jax.shard_map(
        functools.partial(local, mesh.shape["north"], mesh.shape["deep"]),
        mesh=mesh,
        in_specs=placed,
        out_specs=P(None, "north", "deep", None),
        check_vma=False,
    )
```

```python
import functools

import jax
import jax.numpy as jnp
import numpy as np
from jax import lax
from jax.experimental import pallas as pl
from jax.experimental.pallas import tpu as pltpu
from jax.sharding import PartitionSpec as P


VMEM = pltpu.VMEM
F32, BF16 = jnp.float32, jnp.bfloat16
SHARES = (6, 10)


def transform_table(count):
    rank = np.arange(count)
    steps = (2 * rank[:, None] + 1) * (2 * rank[None, :] + 1) % (8 * count)
    table = np.cos(np.pi / (4 * count) * steps) * (2.0 / count) ** 0.5
    high = table.astype(np.float32).astype(BF16)
    low = (table - high.astype(np.float64)).astype(np.float32).astype(BF16)
    return high, low


def split(values):
    high = values.astype(BF16)
    return high, (values - high.astype(F32)).astype(BF16)


def dot(a, b, dims):
    return lax.dot_general(a, b, (dims, ((), ())), preferred_element_type=F32)


def dot3(a, b, dims):
    return dot(a[0], b[0], dims) + (dot(a[0], b[1], dims) + dot(a[1], b[0], dims))


NORTH_KEY = lambda s: s
NEAR_BYTES = 2**20


def near(fits, array):
    return pltpu.with_memory_space_constraint(array, VMEM) if fits else array


def block(fits, shape, dtype=F32):
    return VMEM(shape, dtype) if fits else jax.ShapeDtypeStruct(shape, dtype)


def partner(index, step, count):
    return index ^ step if count & (count - 1) == 0 else lax.rem(index + step, count)


def source(index, step, count):
    return index ^ step if count & (count - 1) == 0 else lax.rem(index + count - step, count)


def call(kernel, outs, cost, memory=None, aliases=None, scratch=(), in_specs=None, out_specs=None):
    flops, moved = cost
    kwargs = {}
    if in_specs is not None:
        kwargs["in_specs"] = in_specs
    if out_specs is not None:
        kwargs["out_specs"] = out_specs
    return pl.pallas_call(
        kernel,
        out_shape=outs,
        input_output_aliases=aliases or {},
        scratch_shapes=scratch,
        cost_estimate=pl.CostEstimate(flops=int(flops), bytes_accessed=int(moved), transcendentals=0),
        **kwargs,
    )


def dot_stacked(a, a_high, b, dims):
    rows = a_high.shape[0]
    both = dot(a, b[0], dims)
    return both[:rows] + (both[rows:] + dot(a_high, b[1], dims))


def x_kernel(inner, outer, chunks, done, *refs):
    field = refs[0]
    total = len(chunks) * outer
    fields, lines = field.shape[:2]
    if done:
        table_ref, before, outs = refs[1], refs[2:-total], refs[-total:]
        table = table_ref[...]
    else:
        high, low = refs[1:3]
        table_ref, outs = refs[-total - 1], refs[-total:]
        before = ()
        me = lax.axis_index("north")
        chip, core = me // inner, lax.rem(me, inner)
        table = jnp.concatenate([ref[partner(chip, s, outer), core] for ref in (high, low) for s in range(outer)], 0)
        table_ref[...] = table
    rows = table.shape[0] // 2
    table_high = table[:rows]
    share = rows // outer
    for old, new in zip(before, outs):
        for r in range(new.shape[0] // ((done + 1) * lines)):
            new[pl.ds(r * (done + 1) * lines, done * lines), :] = old[pl.ds(r * done * lines, done * lines), :]
    pair = 2 if lines % 2 == 0 else 1
    for y in range(0, lines, pair):
        columns = jnp.concatenate([field[f, y + i] for i in range(pair) for f in range(fields)], 0)
        modes = dot_stacked(table, table_high, split(columns), ((1,), (1,)))
        lanes = modes.shape[1] // pair
        for i in range(pair):
            for s in range(outer):
                at = s * share
                for c, count in enumerate(chunks):
                    outs[c * outer + s][pl.ds(done * lines + y + i, count, stride=(done + 1) * lines), :] = modes[
                        at : at + count, i * lanes : (i + 1) * lanes
                    ]
                    at += count


def y_kernel(inner, outer, deep, order, *refs):
    parts, (high, low), outs = refs[:outer], refs[outer : outer + 2], refs[outer + 2 : outer + 2 + deep]
    terms = refs[outer + 2 + deep :]
    me, layer = lax.axis_index("north"), lax.axis_index("deep")
    chip, core = me // inner, lax.rem(me, inner)
    count, share, _ = outs[0].shape
    lines = parts[0].shape[0] // (count * inner)
    table = jnp.concatenate(
        [ref[pl.ds(pl.multiple_of(partner(layer, s, deep) * share, share), share), :] for ref in (high, low) for s in range(deep)],
        0,
    )
    table_high = table[: share * deep]
    lanes = parts[0].shape[1]
    for r in range(count):
        for part, s in zip(parts, (0, *order)):
            for k in range(inner):
                at = (source(chip, s, outer) * inner + source(core, k, inner)) * lines
                at = pl.multiple_of(at, lines)
                for term, value in zip(terms, split(part[pl.ds((r * inner + k) * lines, lines), :])):
                    term[pl.ds(at, lines), r * lanes : (r + 1) * lanes] = value
    for r in range(0, count, 2):
        group = range(r, min(r + 2, count))
        columns = tuple(term[:, r * lanes : (group[-1] + 1) * lanes] for term in terms)
        modes = dot_stacked(table, table_high, columns, ((1,), (0,)))
        for i in group:
            for s in range(deep):
                outs[s][i] = modes[s * share : (s + 1) * share, (i - r) * lanes : (i - r + 1) * lanes]


def z_kernel(fields, steps, deep, start, *refs):
    high, low, factor = refs[len(steps) : len(steps) + 3]
    out, stage, sems = refs[-3:]
    order = tuple(dict.fromkeys(steps))
    parts = [[ref for ref, s in zip(refs, steps) if s == step] for step in order]
    layer = lax.axis_index("deep")
    count, modes_y, lanes = refs[0].shape
    depth = lanes // fields
    table = tuple(
        jnp.concatenate([ref[pl.ds(pl.multiple_of(source(layer, s, deep) * depth, depth), depth), :] for s in order], 0)
        for ref in (high, low)
    )
    rows = count * modes_y
    pieces = [split(sum(ref[...] for ref in part).reshape(rows, lanes)) for part in parts]
    copies = []
    for f in range(fields):
        lines = tuple(
            jnp.concatenate([piece[term][:, f * depth : (f + 1) * depth] for piece in pieces], 1) for term in range(2)
        )
        modes = dot3(lines, table, ((1,), (0,)))
        stage[f] = modes.reshape(count, modes_y, modes.shape[1]) * factor[start : start + count]
        copy = pltpu.make_async_copy(stage.at[f], out.at[f, pl.ds(start, count)], sems.at[f])
        copy.start()
        copies.append(copy)
    for copy in copies:
        copy.wait()


def local(north, deep, forcing, symbol_x, symbol_y, symbol_z):
    fields, size_x, lines, depth = forcing.shape
    size_y, size_z = lines * north, depth * deep
    inner = 2 if north % 2 == 0 else 1
    outer = north // inner
    share_x, share_y = size_x // north, size_y // deep
    lanes = fields * depth
    hold = functools.partial(near, 4 * forcing.size <= NEAR_BYTES)
    made = functools.partial(block, 4 * forcing.size <= NEAR_BYTES)
    ends = np.rint(np.cumsum((0,) + SHARES) / sum(SHARES) * share_x).astype(int)
    chunks = tuple(int(n) for n in np.diff(ends) if n > 0)

    tables = {n: transform_table(n) for n in {size_x, size_y, size_z}}
    table_x = [jnp.asarray(t.reshape(outer, inner, share_x, size_x)) for t in tables[size_x]]
    table_y = [jnp.asarray(t) for t in tables[size_y]]
    table_z = [jnp.asarray(t) for t in tables[size_z]]

    field = jnp.transpose(forcing, (0, 2, 3, 1))
    cost_x = (2 * fields * lines * depth * size_x * outer * share_x * 3, 8 * field.size)
    buffers, ready_x = (), table_x
    for k in range(inner):
        taken = field
        if k:
            pairs = [(j, j // inner * inner + partner_int(j % inner, k, inner)) for j in range(north)]
            taken = hold(lax.ppermute(field, "north", pairs))
        sends = tuple(made((n * (k + 1) * lines, lanes)) for n in chunks for _ in range(outer))
        if k == 0:
            sends = (made((2 * outer * share_x, size_x), BF16),) + sends
        buffers = call(functools.partial(x_kernel, inner, outer, chunks, k), sends, cost_x)(
            taken, *ready_x, *map(hold, buffers)
        )
        if k == 0:
            ready_x, buffers = [hold(buffers[0])], buffers[1:]

    symbol_x, symbol_y, symbol_z, buffers = lax.optimization_barrier((symbol_x, symbol_y, symbol_z, buffers))
    part_x = lax.dynamic_slice_in_dim(symbol_x, lax.axis_index("north") * share_x, share_x)
    part_y = lax.dynamic_slice_in_dim(symbol_y, lax.axis_index("deep") * share_y, share_y)
    symbol = part_x[:, None, None] + part_y[None, :, None] + symbol_z[None, None, :]
    factor = (1.0 - 0.2 * symbol) / (1.0 + 0.2 * symbol)

    north_order = sorted(range(1, outer), key=NORTH_KEY)
    sends_z = deep_sends(deep)
    steps_z = (0,) + tuple(s for s, _ in sends_z)
    result, start = (), 0
    for c, count in enumerate(chunks):
        parts = list(buffers[c * outer : (c + 1) * outer])
        for s in north_order:
            pairs = [(j, partner_int(j // inner, s, outer) * inner + j % inner) for j in range(north)]
            parts[s] = lax.ppermute(parts[s], "north", pairs)
        cost_y = (2 * count * size_y * size_y * lanes * 3, 8 * count * size_y * lanes)
        blocks = call(
            functools.partial(y_kernel, inner, outer, deep, north_order),
            tuple(made((count, share_y, lanes)) for _ in range(deep)),
            cost_y,
            scratch=(VMEM((size_y, count * lanes), BF16), VMEM((size_y, count * lanes), BF16)),
        )(*[hold(parts[s]) for s in (0, *north_order)], *map(hold, table_y))
        gathered = [blocks[0]] + [lax.ppermute(blocks[s], "deep", pairs) for s, pairs in sends_z]
        shape = (fields, share_x, share_y, size_z)
        cost_z = (2 * count * share_y * size_z * size_z * fields * 3, 8 * count * share_y * size_z * fields)
        whole = pl.BlockSpec(memory_space=VMEM)
        anywhere = pl.BlockSpec(memory_space=pl.ANY)
        result = (
            call(
                functools.partial(z_kernel, fields, steps_z, deep, start),
                jax.ShapeDtypeStruct(shape, F32),
                cost_z,
                aliases={len(steps_z) + 3: 0} if c else {},
                scratch=(VMEM((fields, count) + shape[2:], F32), pltpu.SemaphoreType.DMA((fields,))),
                in_specs=[whole] * (len(steps_z) + 3) + [anywhere] * len(result),
                out_specs=anywhere,
            )(*map(hold, gathered), *map(hold, table_z), hold(factor), *result),
        )
        start += count
    return result[0]


def partner_int(index, step, count):
    return index ^ step if count & (count - 1) == 0 else (index + step) % count


def deep_sends(deep):
    steps = [(s, [(j, partner_int(j, s, deep)) for j in range(deep)]) for s in range(1, deep)]
    if deep != 4:
        return sorted(steps, key=lambda step: (-step[0].bit_length(), step[0]))
    (one, near), (two, across), (three, ends) = steps
    return [(two, across), (three, ends), (one, near)]


def solution(mesh):
    placed = (P(None, None, "north", "deep"), P(), P(), P())
    return jax.shard_map(
        functools.partial(local, mesh.shape["north"], mesh.shape["deep"]),
        mesh=mesh,
        in_specs=placed,
        out_specs=P(None, "north", "deep", None),
        check_vma=False,
    )
```

```python
import functools

import jax
import jax.numpy as jnp
import numpy as np
from jax import lax
from jax.experimental import pallas as pl
from jax.experimental.pallas import tpu as pltpu
from jax.sharding import PartitionSpec as P


VMEM = pltpu.VMEM
F32, BF16 = jnp.float32, jnp.bfloat16
SHARES = (6, 10)


def transform_table(count):
    rank = np.arange(count)
    steps = (2 * rank[:, None] + 1) * (2 * rank[None, :] + 1) % (8 * count)
    table = np.cos(np.pi / (4 * count) * steps) * (2.0 / count) ** 0.5
    high = table.astype(np.float32).astype(BF16)
    low = (table - high.astype(np.float64)).astype(np.float32).astype(BF16)
    return high, low


def split(values):
    high = values.astype(BF16)
    return high, (values - high.astype(F32)).astype(BF16)


def dot(a, b, dims):
    return lax.dot_general(a, b, (dims, ((), ())), preferred_element_type=F32)


def dot3(a, b, dims):
    return dot(a[0], b[0], dims) + (dot(a[0], b[1], dims) + dot(a[1], b[0], dims))


NORTH_KEY = (lambda s: s, lambda s: s)
NEAR_BYTES = 2**20


def near(fits, array):
    return pltpu.with_memory_space_constraint(array, VMEM) if fits else array


def block(fits, shape, dtype=F32):
    return VMEM(shape, dtype) if fits else jax.ShapeDtypeStruct(shape, dtype)


def partner(index, step, count):
    return index ^ step if count & (count - 1) == 0 else lax.rem(index + step, count)


def source(index, step, count):
    return index ^ step if count & (count - 1) == 0 else lax.rem(index + count - step, count)


def call(kernel, outs, cost, aliases=None, scratch=(), in_specs=None, out_specs=None):
    flops, moved = cost
    kwargs = {}
    if in_specs is not None:
        kwargs["in_specs"] = in_specs
    if out_specs is not None:
        kwargs["out_specs"] = out_specs
    return pl.pallas_call(
        kernel,
        out_shape=outs,
        input_output_aliases=aliases or {},
        scratch_shapes=scratch,
        cost_estimate=pl.CostEstimate(flops=int(flops), bytes_accessed=int(moved), transcendentals=0),
        **kwargs,
    )


def dot_stacked(a, a_high, b, dims):
    rows = a_high.shape[0]
    both = dot(a, b[0], dims)
    return both[:rows] + (both[rows:] + dot(a_high, b[1], dims))


def x_kernel(inner, outer, chunks, *refs):
    field, high, low = refs[:3]
    tables, outs = refs[3 : 3 + len(chunks)], refs[3 + len(chunks) :]
    me = lax.axis_index("north")
    chip, core = me // inner, lax.rem(me, inner)
    shares = [ref[partner(chip, s, outer), core] for ref in (high, low) for s in range(outer)]
    table = jnp.concatenate(shares, 0).astype(BF16)
    for (first, last, _, _), ref in zip(chunks, tables):
        ref[...] = jnp.concatenate([rows[first:last] for rows in shares], 0).astype(BF16)
    for y, s, value in line_modes(field, table, outer):
        for c, (_, _, start, count) in enumerate(chunks):
            outs[c * outer + s][pl.ds(y, count, stride=field.shape[1]), :] = value[start : start + count]


def line_modes(field, table, outer):
    fields, lines = field.shape[:2]
    rows = table.shape[0] // 2
    share = rows // outer
    table_high = table[:rows]
    pair = 2 if lines % 2 == 0 else 1
    for y in range(0, lines, pair):
        columns = jnp.concatenate([field[f, y + i] for i in range(pair) for f in range(fields)], 0)
        modes = dot_stacked(table, table_high, split(columns), ((1,), (1,)))
        lanes = modes.shape[1] // pair
        for i in range(pair):
            for s in range(outer):
                yield y + i, s, modes[s * share : (s + 1) * share, i * lanes : (i + 1) * lanes]


def other_kernel(outer, count, skip, *refs):
    field, table, before, outs = refs[0], refs[1], refs[2:-outer], refs[-outer:]
    lines = field.shape[1]
    done = before[0].shape[0] // (count * lines) if before else 0
    join(count, [before], outs)
    for y, s, value in line_modes(field, table[...], outer):
        outs[s][pl.ds(done * lines + y, count, stride=(done + 1) * lines), :] = value[skip : skip + count]


def join(count, groups, outs):
    total = outs[0].shape[0] // count
    at = 0
    for blocks in groups:
        for block, out in zip(blocks, outs):
            size = block.shape[0] // count
            for r in range(count):
                out[pl.ds(r * total + at, size), :] = block[pl.ds(r * size, size), :]
        at += blocks[0].shape[0] // count if blocks else 0


def join_kernel(count, outer, *refs):
    join(count, (refs[:outer], refs[outer : 2 * outer]), refs[2 * outer :])


def y_kernel(inner, outer, deep, order, *refs):
    parts, (high, low), outs = refs[:outer], refs[outer : outer + 2], refs[outer + 2 : outer + 2 + deep]
    terms = refs[outer + 2 + deep :]
    me, layer = lax.axis_index("north"), lax.axis_index("deep")
    chip, core = me // inner, lax.rem(me, inner)
    count, share, _ = outs[0].shape
    lines = parts[0].shape[0] // (count * inner)
    table = jnp.concatenate(
        [ref[pl.ds(pl.multiple_of(partner(layer, s, deep) * share, share), share), :] for ref in (high, low) for s in range(deep)],
        0,
    )
    table_high = table[: share * deep]
    lanes = parts[0].shape[1]
    for r in range(count):
        for part, s in zip(parts, (0, *order)):
            for k in range(inner):
                at = (source(chip, s, outer) * inner + source(core, k, inner)) * lines
                at = pl.multiple_of(at, lines)
                for term, value in zip(terms, split(part[pl.ds((r * inner + k) * lines, lines), :])):
                    term[pl.ds(at, lines), r * lanes : (r + 1) * lanes] = value
    for r in range(0, count, 2):
        group = range(r, min(r + 2, count))
        columns = tuple(term[:, r * lanes : (group[-1] + 1) * lanes] for term in terms)
        modes = dot_stacked(table, table_high, columns, ((1,), (0,)))
        for i in group:
            for s in range(deep):
                outs[s][i] = modes[s * share : (s + 1) * share, (i - r) * lanes : (i - r + 1) * lanes]


def z_kernel(fields, steps, deep, start, *refs):
    high, low, factor = refs[len(steps) : len(steps) + 3]
    out, stage, sems = refs[-3:]
    order = tuple(dict.fromkeys(steps))
    parts = [[ref for ref, s in zip(refs, steps) if s == step] for step in order]
    layer = lax.axis_index("deep")
    count, modes_y, lanes = refs[0].shape
    depth = lanes // fields
    table = tuple(
        jnp.concatenate([ref[pl.ds(pl.multiple_of(source(layer, s, deep) * depth, depth), depth), :] for s in order], 0)
        for ref in (high, low)
    )
    rows = count * modes_y
    pieces = [split(sum(ref[...] for ref in part).reshape(rows, lanes)) for part in parts]
    copies = []
    for f in range(fields):
        lines = tuple(
            jnp.concatenate([piece[term][:, f * depth : (f + 1) * depth] for piece in pieces], 1) for term in range(2)
        )
        modes = dot3(lines, table, ((1,), (0,)))
        stage[f] = modes.reshape(count, modes_y, modes.shape[1]) * factor[start : start + count]
        copy = pltpu.make_async_copy(stage.at[f], out.at[f, pl.ds(start, count)], sems.at[f])
        copy.start()
        copies.append(copy)
    for copy in copies:
        copy.wait()


def local(north, deep, forcing, symbol_x, symbol_y, symbol_z):
    fields, size_x, lines, depth = forcing.shape
    size_y, size_z = lines * north, depth * deep
    inner = 2 if north % 2 == 0 else 1
    outer = north // inner
    share_x, share_y = size_x // north, size_y // deep
    lanes = fields * depth
    hold = functools.partial(near, 4 * forcing.size <= NEAR_BYTES)
    made = functools.partial(block, 4 * forcing.size <= NEAR_BYTES)
    ends = np.rint(np.cumsum((0,) + SHARES) / sum(SHARES) * share_x).astype(int)
    chunks = tuple(int(n) for n in np.diff(ends) if n > 0)

    tables = {n: transform_table(n) for n in {size_x, size_y, size_z}}
    table_x = [jnp.asarray(t.astype(np.float32).reshape(outer, inner, share_x, size_x)) for t in tables[size_x]]
    table_y = [jnp.asarray(t) for t in tables[size_y]]
    table_z = [jnp.asarray(t) for t in tables[size_z]]

    field = jnp.transpose(forcing, (0, 2, 3, 1))
    cost_x = (2 * field.size * outer * share_x * 3, 8 * field.size)
    spans, start = [], 0
    for count in chunks:
        spans.append((start // 8 * 8, min(-(-(start + count) // 8) * 8, share_x), start, count))
        start += count
    sends = [made((2 * outer * (last - first), size_x), BF16) for first, last, _, _ in spans]
    sends += [made((count * lines, lanes)) for count in chunks for _ in range(outer)]
    own = call(functools.partial(x_kernel, inner, outer, spans), tuple(sends), cost_x)(field, *table_x)
    ready_x, own = own[: len(chunks)], own[len(chunks) :]
    buffers = [own[c * outer : (c + 1) * outer] for c in range(len(chunks))]
    for k in range(1, inner):
        pairs = [(j, j // inner * inner + partner_int(j % inner, k, inner)) for j in range(north)]
        taken = hold(lax.ppermute(field, "north", pairs))
        for c, (first, last, start, count) in enumerate(spans):
            together = buffers[c] if c == 0 else ()
            other = call(
                functools.partial(other_kernel, outer, count, start - first),
                tuple(made((count * (k + 1 if together else 1) * lines, lanes)) for _ in range(outer)),
                (cost_x[0] * count // share_x, cost_x[1]),
            )(taken, hold(ready_x[c]), *map(hold, together))
            if not together:
                other = call(
                    functools.partial(join_kernel, count, outer),
                    tuple(made((count * (k + 1) * lines, lanes)) for _ in range(outer)),
                    (1000, 16 * outer * count * lines * lanes),
                )(*map(hold, buffers[c]), *map(hold, other))
            buffers[c] = other

    symbol_x, symbol_y, symbol_z, buffers[0] = lax.optimization_barrier((symbol_x, symbol_y, symbol_z, buffers[0]))
    part_x = lax.dynamic_slice_in_dim(symbol_x, lax.axis_index("north") * share_x, share_x)
    part_y = lax.dynamic_slice_in_dim(symbol_y, lax.axis_index("deep") * share_y, share_y)
    symbol = part_x[:, None, None] + part_y[None, :, None] + symbol_z[None, None, :]
    factor = (1.0 - 0.2 * symbol) / (1.0 + 0.2 * symbol)

    result, start = (), 0
    for c, count in enumerate(chunks):
        north_order = sorted(range(1, outer), key=NORTH_KEY[min(c, 1)])
        parts = list(buffers[c])
        for s in north_order:
            pairs = [(j, partner_int(j // inner, s, outer) * inner + j % inner) for j in range(north)]
            parts[s] = lax.ppermute(parts[s], "north", pairs)
        cost_y = (2 * count * size_y * size_y * lanes * 3, 8 * count * size_y * lanes)
        blocks = call(
            functools.partial(y_kernel, inner, outer, deep, north_order),
            tuple(made((count, share_y, lanes)) for _ in range(deep)),
            cost_y,
            scratch=(VMEM((size_y, count * lanes), BF16), VMEM((size_y, count * lanes), BF16)),
        )(*[hold(parts[s]) for s in (0, *north_order)], *map(hold, table_y))
        sends_z = deep_sends(deep, c)
        steps_z = (0,) + tuple(s for s, _ in sends_z)
        gathered = [blocks[0]] + [lax.ppermute(blocks[s], "deep", pairs) for s, pairs in sends_z]
        shape = (fields, share_x, share_y, size_z)
        cost_z = (2 * count * share_y * size_z * size_z * fields * 3, 8 * count * share_y * size_z * fields)
        whole = pl.BlockSpec(memory_space=VMEM)
        anywhere = pl.BlockSpec(memory_space=pl.ANY)
        result = (
            call(
                functools.partial(z_kernel, fields, steps_z, deep, start),
                jax.ShapeDtypeStruct(shape, F32),
                cost_z,
                aliases={len(steps_z) + 3: 0} if c else {},
                scratch=(VMEM((fields, count) + shape[2:], F32), pltpu.SemaphoreType.DMA((fields,))),
                in_specs=[whole] * (len(steps_z) + 3) + [anywhere] * len(result),
                out_specs=anywhere,
            )(*map(hold, gathered), *map(hold, table_z), hold(factor), *result),
        )
        start += count
    return result[0]


def partner_int(index, step, count):
    return index ^ step if count & (count - 1) == 0 else (index + step) % count


def deep_sends(deep, chunk):
    steps = [(s, [(j, partner_int(j, s, deep)) for j in range(deep)]) for s in range(1, deep)]
    if deep != 4:
        return sorted(steps, key=lambda step: (-step[0].bit_length(), step[0]))
    (one, near), (two, across), (three, ends) = steps
    return [[(three, ends), (two, across), (one, near)], [(two, across), (three, ends), (one, near)]][min(chunk, 1)]


def solution(mesh):
    def step(*arrays):
        return local(mesh.shape["north"], mesh.shape["deep"], *arrays)

    placed = (P(None, None, "north", "deep"), P(), P(), P())
    return jax.shard_map(
        step, mesh=mesh, in_specs=placed, out_specs=P(None, "north", "deep", None), check_vma=False
    )
```

```python
import functools

import jax
import jax.numpy as jnp
import numpy as np
from jax import lax
from jax.experimental import pallas as pl
from jax.experimental.pallas import tpu as pltpu
from jax.sharding import PartitionSpec as P


VMEM = pltpu.VMEM
F32, BF16 = jnp.float32, jnp.bfloat16
SHARES = (6, 10)


def transform_table(count):
    rank = np.arange(count)
    steps = (2 * rank[:, None] + 1) * (2 * rank[None, :] + 1) % (8 * count)
    table = np.cos(np.pi / (4 * count) * steps) * (2.0 / count) ** 0.5
    high = table.astype(np.float32).astype(BF16)
    low = (table - high.astype(np.float64)).astype(np.float32).astype(BF16)
    return high, low


def split(values):
    high = values.astype(BF16)
    return high, (values - high.astype(F32)).astype(BF16)


def dot(a, b, dims):
    return lax.dot_general(a, b, (dims, ((), ())), preferred_element_type=F32)


def dot3(a, b, dims):
    return dot(a[0], b[0], dims) + (dot(a[0], b[1], dims) + dot(a[1], b[0], dims))


NORTH_KEY = (lambda s: s, lambda s: s)
NEAR_BYTES = 2**20


def near(fits, array):
    return pltpu.with_memory_space_constraint(array, VMEM) if fits else array


def block(fits, shape, dtype=F32):
    return VMEM(shape, dtype) if fits else jax.ShapeDtypeStruct(shape, dtype)


def partner(index, step, count):
    return index ^ step if count & (count - 1) == 0 else lax.rem(index + step, count)


def source(index, step, count):
    return index ^ step if count & (count - 1) == 0 else lax.rem(index + count - step, count)


def call(kernel, outs, cost, aliases=None, scratch=(), in_specs=None, out_specs=None):
    flops, moved = cost
    kwargs = {}
    if in_specs is not None:
        kwargs["in_specs"] = in_specs
    if out_specs is not None:
        kwargs["out_specs"] = out_specs
    return pl.pallas_call(
        kernel,
        out_shape=outs,
        input_output_aliases=aliases or {},
        scratch_shapes=scratch,
        cost_estimate=pl.CostEstimate(flops=int(flops), bytes_accessed=int(moved), transcendentals=0),
        **kwargs,
    )


def stack_terms(high, low):
    return jnp.concatenate(
        [jnp.concatenate([high, high], 1), jnp.concatenate([low, jnp.zeros_like(low)], 1)], 0
    )


def dot_stacked(stacked, columns, dims):
    rows = stacked.shape[0] // 2
    both = dot(stacked, columns, dims)
    return both[:rows] + both[rows:]


def x_kernel(inner, outer, chunks, *refs):
    field, high, low = refs[:3]
    tables, outs = refs[3 : 3 + len(chunks)], refs[3 + len(chunks) :]
    me = lax.axis_index("north")
    chip, core = me // inner, lax.rem(me, inner)
    shares = [[ref[partner(chip, s, outer), core] for s in range(outer)] for ref in (high, low)]
    table = stack_terms(*(jnp.concatenate(term, 0).astype(BF16) for term in shares))
    for (first, last, _, _), ref in zip(chunks, tables):
        ref[...] = stack_terms(*(jnp.concatenate([rows[first:last] for rows in term], 0).astype(BF16) for term in shares))
    for y, s, value in line_modes(field, table, outer):
        for c, (_, _, start, count) in enumerate(chunks):
            outs[c * outer + s][pl.ds(y, count, stride=field.shape[1]), :] = value[start : start + count]


def line_modes(field, table, outer):
    fields, lines = field.shape[:2]
    rows = table.shape[0] // 2
    share = rows // outer
    pair = 2 if lines % 2 == 0 else 1
    for y in range(0, lines, pair):
        columns = jnp.concatenate([field[f, y + i] for i in range(pair) for f in range(fields)], 0)
        modes = dot_stacked(table, jnp.concatenate(split(columns), 1), ((1,), (1,)))
        lanes = modes.shape[1] // pair
        for i in range(pair):
            for s in range(outer):
                yield y + i, s, modes[s * share : (s + 1) * share, i * lanes : (i + 1) * lanes]


def other_kernel(outer, count, skip, *refs):
    field, table, before, outs = refs[0], refs[1], refs[2:-outer], refs[-outer:]
    lines = field.shape[1]
    done = before[0].shape[0] // (count * lines) if before else 0
    join(count, [before], outs)
    for y, s, value in line_modes(field, table[...], outer):
        outs[s][pl.ds(done * lines + y, count, stride=(done + 1) * lines), :] = value[skip : skip + count]


def join(count, groups, outs):
    total = outs[0].shape[0] // count
    at = 0
    for blocks in groups:
        for block, out in zip(blocks, outs):
            size = block.shape[0] // count
            for r in range(count):
                out[pl.ds(r * total + at, size), :] = block[pl.ds(r * size, size), :]
        at += blocks[0].shape[0] // count if blocks else 0


def join_kernel(count, outer, *refs):
    join(count, (refs[:outer], refs[outer : 2 * outer]), refs[2 * outer :])


def y_kernel(inner, outer, deep, order, *refs):
    parts, (high, low), outs = refs[:outer], refs[outer : outer + 2], refs[outer + 2 : outer + 2 + deep]
    terms, total = refs[-1], refs[-1].shape[0] // 2
    me, layer = lax.axis_index("north"), lax.axis_index("deep")
    chip, core = me // inner, lax.rem(me, inner)
    count, share, _ = outs[0].shape
    lines = parts[0].shape[0] // (count * inner)
    table = stack_terms(
        *(
            jnp.concatenate([ref[pl.ds(pl.multiple_of(partner(layer, s, deep) * share, share), share), :] for s in range(deep)], 0)
            for ref in (high, low)
        )
    )
    lanes = parts[0].shape[1]
    for r in range(count):
        for part, s in zip(parts, (0, *order)):
            for k in range(inner):
                at = (source(chip, s, outer) * inner + source(core, k, inner)) * lines
                at = pl.multiple_of(at, lines)
                for term, value in enumerate(split(part[pl.ds((r * inner + k) * lines, lines), :])):
                    terms[pl.ds(at + term * total, lines), r * lanes : (r + 1) * lanes] = value
    for r in range(0, count, 2):
        group = range(r, min(r + 2, count))
        modes = dot_stacked(table, terms[:, r * lanes : (group[-1] + 1) * lanes], ((1,), (0,)))
        for i in group:
            for s in range(deep):
                outs[s][i] = modes[s * share : (s + 1) * share, (i - r) * lanes : (i - r + 1) * lanes]


def z_kernel(fields, steps, deep, start, *refs):
    high, low, factor = refs[len(steps) : len(steps) + 3]
    out, stage, sems = refs[-3:]
    order = tuple(dict.fromkeys(steps))
    parts = [[ref for ref, s in zip(refs, steps) if s == step] for step in order]
    layer = lax.axis_index("deep")
    count, modes_y, lanes = refs[0].shape
    depth = lanes // fields
    table = tuple(
        jnp.concatenate([ref[pl.ds(pl.multiple_of(source(layer, s, deep) * depth, depth), depth), :] for s in order], 0)
        for ref in (high, low)
    )
    rows = count * modes_y
    pieces = [split(sum(ref[...] for ref in part).reshape(rows, lanes)) for part in parts]
    copies = []
    for f in range(fields):
        lines = tuple(
            jnp.concatenate([piece[term][:, f * depth : (f + 1) * depth] for piece in pieces], 1) for term in range(2)
        )
        modes = dot3(lines, table, ((1,), (0,)))
        stage[f] = modes.reshape(count, modes_y, modes.shape[1]) * factor[start : start + count]
        copy = pltpu.make_async_copy(stage.at[f], out.at[f, pl.ds(start, count)], sems.at[f])
        copy.start()
        copies.append(copy)
    for copy in copies:
        copy.wait()


def local(north, deep, forcing, symbol_x, symbol_y, symbol_z):
    fields, size_x, lines, depth = forcing.shape
    size_y, size_z = lines * north, depth * deep
    inner = 2 if north % 2 == 0 else 1
    outer = north // inner
    share_x, share_y = size_x // north, size_y // deep
    lanes = fields * depth
    hold = functools.partial(near, 4 * forcing.size <= NEAR_BYTES)
    made = functools.partial(block, 4 * forcing.size <= NEAR_BYTES)
    ends = np.rint(np.cumsum((0,) + SHARES) / sum(SHARES) * share_x).astype(int)
    chunks = tuple(int(n) for n in np.diff(ends) if n > 0)

    tables = {n: transform_table(n) for n in {size_x, size_y, size_z}}
    table_x = [jnp.asarray(t.astype(np.float32).reshape(outer, inner, share_x, size_x)) for t in tables[size_x]]
    table_y = [jnp.asarray(t) for t in tables[size_y]]
    table_z = [jnp.asarray(t) for t in tables[size_z]]

    field = jnp.transpose(forcing, (0, 2, 3, 1))
    cost_x = (2 * field.size * outer * share_x * 3, 8 * field.size)
    spans, start = [], 0
    for count in chunks:
        spans.append((start // 8 * 8, min(-(-(start + count) // 8) * 8, share_x), start, count))
        start += count
    sends = [made((2 * outer * (last - first), 2 * size_x), BF16) for first, last, _, _ in spans]
    sends += [made((count * lines, lanes)) for count in chunks for _ in range(outer)]
    own = call(functools.partial(x_kernel, inner, outer, spans), tuple(sends), cost_x)(field, *table_x)
    ready_x, own = own[: len(chunks)], own[len(chunks) :]
    buffers = [own[c * outer : (c + 1) * outer] for c in range(len(chunks))]
    for k in range(1, inner):
        pairs = [(j, j // inner * inner + partner_int(j % inner, k, inner)) for j in range(north)]
        taken = hold(lax.ppermute(field, "north", pairs))
        for c, (first, last, start, count) in enumerate(spans):
            together = buffers[c] if c == 0 else ()
            other = call(
                functools.partial(other_kernel, outer, count, start - first),
                tuple(made((count * (k + 1 if together else 1) * lines, lanes)) for _ in range(outer)),
                (cost_x[0] * count // share_x, cost_x[1]),
            )(taken, hold(ready_x[c]), *map(hold, together))
            if not together:
                other = call(
                    functools.partial(join_kernel, count, outer),
                    tuple(made((count * (k + 1) * lines, lanes)) for _ in range(outer)),
                    (1000, 16 * outer * count * lines * lanes),
                )(*map(hold, buffers[c]), *map(hold, other))
            buffers[c] = other

    received = []
    for c, count in enumerate(chunks):
        north_order = sorted(range(1, outer), key=NORTH_KEY[min(c, 1)])
        parts = list(buffers[c])
        for s in north_order:
            pairs = [(j, partner_int(j // inner, s, outer) * inner + j % inner) for j in range(north)]
            parts[s] = lax.ppermute(parts[s], "north", pairs)
        cost_y = (2 * count * size_y * size_y * lanes * 3, 8 * count * size_y * lanes)
        blocks = call(
            functools.partial(y_kernel, inner, outer, deep, north_order),
            tuple(made((count, share_y, lanes)) for _ in range(deep)),
            cost_y,
            scratch=(VMEM((2 * size_y, count * lanes), BF16),),
        )(*[hold(parts[s]) for s in (0, *north_order)], *map(hold, table_y))
        sends_z = deep_sends(deep, c)
        steps_z = (0,) + tuple(s for s, _ in sends_z)
        gathered = [blocks[0]] + [lax.ppermute(blocks[s], "deep", pairs) for s, pairs in sends_z]
        received.append((steps_z, gathered, blocks))

    symbol_x, symbol_y, symbol_z, _ = lax.optimization_barrier((symbol_x, symbol_y, symbol_z, received[-1][2]))
    part_x = lax.dynamic_slice_in_dim(symbol_x, lax.axis_index("north") * share_x, share_x)
    part_y = lax.dynamic_slice_in_dim(symbol_y, lax.axis_index("deep") * share_y, share_y)
    symbol = part_x[:, None, None] + part_y[None, :, None] + symbol_z[None, None, :]
    factor = (1.0 - 0.2 * symbol) / (1.0 + 0.2 * symbol)

    result, start = (), 0
    for c, (count, (steps_z, gathered, _)) in enumerate(zip(chunks, received)):
        shape = (fields, share_x, share_y, size_z)
        cost_z = (2 * count * share_y * size_z * size_z * fields * 3, 8 * count * share_y * size_z * fields)
        whole = pl.BlockSpec(memory_space=VMEM)
        anywhere = pl.BlockSpec(memory_space=pl.ANY)
        result = (
            call(
                functools.partial(z_kernel, fields, steps_z, deep, start),
                jax.ShapeDtypeStruct(shape, F32),
                cost_z,
                aliases={len(steps_z) + 3: 0} if c else {},
                scratch=(VMEM((fields, count) + shape[2:], F32), pltpu.SemaphoreType.DMA((fields,))),
                in_specs=[whole] * (len(steps_z) + 3) + [anywhere] * len(result),
                out_specs=anywhere,
            )(*map(hold, gathered), *map(hold, table_z), hold(factor), *result),
        )
        start += count
    return result[0]


def partner_int(index, step, count):
    return index ^ step if count & (count - 1) == 0 else (index + step) % count


def deep_sends(deep, chunk):
    steps = [(s, [(j, partner_int(j, s, deep)) for j in range(deep)]) for s in range(1, deep)]
    if deep != 4:
        return sorted(steps, key=lambda step: (-step[0].bit_length(), step[0]))
    (one, near), (two, across), (three, ends) = steps
    return [[(three, ends), (two, across), (one, near)], [(two, across), (three, ends), (one, near)]][min(chunk, 1)]


def solution(mesh):
    def step(*arrays):
        return local(mesh.shape["north"], mesh.shape["deep"], *arrays)

    placed = (P(None, None, "north", "deep"), P(), P(), P())
    return jax.shard_map(
        step, mesh=mesh, in_specs=placed, out_specs=P(None, "north", "deep", None), check_vma=False
    )
```

```python
import functools

import jax
import jax.numpy as jnp
import numpy as np
from jax import lax
from jax.experimental import pallas as pl
from jax.experimental.pallas import tpu as pltpu
from jax.sharding import PartitionSpec as P


VMEM = pltpu.VMEM
F32, BF16 = jnp.float32, jnp.bfloat16
SHARES = (6, 10)


def transform_table(count):
    rank = np.arange(count)
    steps = (2 * rank[:, None] + 1) * (2 * rank[None, :] + 1) % (8 * count)
    table = np.cos(np.pi / (4 * count) * steps) * (2.0 / count) ** 0.5
    high = table.astype(np.float32).astype(BF16)
    low = (table - high.astype(np.float64)).astype(np.float32).astype(BF16)
    return high, low


def split(values):
    high = values.astype(BF16)
    return high, (values - high.astype(F32)).astype(BF16)


def dot(a, b, dims):
    return lax.dot_general(a, b, (dims, ((), ())), preferred_element_type=F32)


def dot3(a, b, dims):
    return dot(a[0], b[0], dims) + (dot(a[0], b[1], dims) + dot(a[1], b[0], dims))


CUTS = 2
NORTH_KEY = (lambda s: s, lambda s: s)
NEAR_BYTES = 2**20


def near(fits, array):
    return pltpu.with_memory_space_constraint(array, VMEM) if fits else array


def block(fits, shape, dtype=F32):
    return VMEM(shape, dtype) if fits else jax.ShapeDtypeStruct(shape, dtype)


def partner(index, step, count):
    return index ^ step if count & (count - 1) == 0 else lax.rem(index + step, count)


def source(index, step, count):
    return index ^ step if count & (count - 1) == 0 else lax.rem(index + count - step, count)


def call(kernel, outs, cost, aliases=None, scratch=(), in_specs=None, out_specs=None):
    flops, moved = cost
    kwargs = {}
    if in_specs is not None:
        kwargs["in_specs"] = in_specs
    if out_specs is not None:
        kwargs["out_specs"] = out_specs
    return pl.pallas_call(
        kernel,
        out_shape=outs,
        input_output_aliases=aliases or {},
        scratch_shapes=scratch,
        cost_estimate=pl.CostEstimate(flops=int(flops), bytes_accessed=int(moved), transcendentals=0),
        **kwargs,
    )


def stack_terms(high, low):
    return jnp.concatenate(
        [jnp.concatenate([high, high], 1), jnp.concatenate([low, jnp.zeros_like(low)], 1)], 0
    )


def dot_stacked(stacked, columns, dims):
    rows = stacked.shape[0] // 2
    both = dot(stacked, columns, dims)
    return both[:rows] + both[rows:]


def x_kernel(inner, outer, chunks, *refs):
    field, high, low = refs[:3]
    tables, outs = refs[3 : 3 + len(chunks)], refs[3 + len(chunks) :]
    me = lax.axis_index("north")
    chip, core = me // inner, lax.rem(me, inner)
    shares = [[ref[partner(chip, s, outer), core] for s in range(outer)] for ref in (high, low)]
    table = stack_terms(*(jnp.concatenate(term, 0).astype(BF16) for term in shares))
    for (first, last, _, _), ref in zip(chunks, tables):
        ref[...] = stack_terms(*(jnp.concatenate([rows[first:last] for rows in term], 0).astype(BF16) for term in shares))
    for y, s, value in line_modes(field, table, outer):
        for c, (_, _, start, count) in enumerate(chunks):
            outs[c * outer + s][pl.ds(y, count, stride=field.shape[1]), :] = value[start : start + count]


def line_modes(field, table, outer):
    fields, lines = field.shape[:2]
    rows = table.shape[0] // 2
    share = rows // outer
    pair = 2 if lines % 2 == 0 else 1
    for y in range(0, lines, pair):
        columns = jnp.concatenate([field[f, y + i] for i in range(pair) for f in range(fields)], 0)
        modes = dot_stacked(table, jnp.concatenate(split(columns), 1), ((1,), (1,)))
        lanes = modes.shape[1] // pair
        for i in range(pair):
            for s in range(outer):
                yield y + i, s, modes[s * share : (s + 1) * share, i * lanes : (i + 1) * lanes]


def other_kernel(outer, count, skip, *refs):
    field, table, before, outs = refs[0], refs[1], refs[2:-outer], refs[-outer:]
    lines = field.shape[1]
    done = before[0].shape[0] // (count * lines) if before else 0
    join(count, [before], outs)
    for y, s, value in line_modes(field, table[...], outer):
        outs[s][pl.ds(done * lines + y, count, stride=(done + 1) * lines), :] = value[skip : skip + count]


def join(count, groups, outs):
    total = outs[0].shape[0] // count
    at = 0
    for blocks in groups:
        for block, out in zip(blocks, outs):
            size = block.shape[0] // count
            for r in range(count):
                out[pl.ds(r * total + at, size), :] = block[pl.ds(r * size, size), :]
        at += blocks[0].shape[0] // count if blocks else 0


def join_kernel(count, outer, *refs):
    join(count, (refs[:outer], refs[outer : 2 * outer]), refs[2 * outer :])


def y_kernel(inner, outer, deep, order, *refs):
    parts, (high, low), outs = refs[:outer], refs[outer : outer + 2], refs[outer + 2 : outer + 2 + deep]
    terms, total = refs[-1], refs[-1].shape[0] // 2
    me, layer = lax.axis_index("north"), lax.axis_index("deep")
    chip, core = me // inner, lax.rem(me, inner)
    count, share, _ = outs[0].shape
    lines = parts[0].shape[0] // (count * inner)
    table = stack_terms(
        *(
            jnp.concatenate([ref[pl.ds(pl.multiple_of(partner(layer, s, deep) * share, share), share), :] for s in range(deep)], 0)
            for ref in (high, low)
        )
    )
    lanes = parts[0].shape[1]
    for r in range(count):
        for part, s in zip(parts, (0, *order)):
            for k in range(inner):
                at = (source(chip, s, outer) * inner + source(core, k, inner)) * lines
                at = pl.multiple_of(at, lines)
                for term, value in enumerate(split(part[pl.ds((r * inner + k) * lines, lines), :])):
                    terms[pl.ds(at + term * total, lines), r * lanes : (r + 1) * lanes] = value
    for r in range(0, count, 2):
        group = range(r, min(r + 2, count))
        modes = dot_stacked(table, terms[:, r * lanes : (group[-1] + 1) * lanes], ((1,), (0,)))
        for i in group:
            for s in range(deep):
                outs[s][i] = modes[s * share : (s + 1) * share, (i - r) * lanes : (i - r + 1) * lanes]


def z_kernel(fields, steps, deep, start, *refs):
    high, low, factor = refs[len(steps) : len(steps) + 3]
    out, stage, sems = refs[-3:]
    order = tuple(dict.fromkeys(steps))
    parts = [[ref for ref, s in zip(refs, steps) if s == step] for step in order]
    layer = lax.axis_index("deep")
    count, modes_y, lanes = refs[0].shape
    depth = lanes // fields
    table = tuple(
        jnp.concatenate([ref[pl.ds(pl.multiple_of(source(layer, s, deep) * depth, depth), depth), :] for s in order], 0)
        for ref in (high, low)
    )
    rows = count * modes_y
    pieces = [split(sum(ref[...] for ref in part).reshape(rows, lanes)) for part in parts]
    copies = []
    for f in range(fields):
        lines = tuple(
            jnp.concatenate([piece[term][:, f * depth : (f + 1) * depth] for piece in pieces], 1) for term in range(2)
        )
        for i in range(CUTS):
            first, last = count * i // CUTS, count * (i + 1) // CUTS
            part = tuple(term[first * modes_y : last * modes_y] for term in lines)
            modes = dot3(part, table, ((1,), (0,)))
            stage[f, first:last] = modes.reshape(last - first, modes_y, modes.shape[1]) * factor[start + first : start + last]
            copy = pltpu.make_async_copy(
                stage.at[f, pl.ds(first, last - first)], out.at[f, pl.ds(start + first, last - first)], sems.at[f, i]
            )
            copy.start()
            copies.append(copy)
    for copy in copies:
        copy.wait()


def local(north, deep, forcing, symbol_x, symbol_y, symbol_z):
    fields, size_x, lines, depth = forcing.shape
    size_y, size_z = lines * north, depth * deep
    inner = 2 if north % 2 == 0 else 1
    outer = north // inner
    share_x, share_y = size_x // north, size_y // deep
    lanes = fields * depth
    hold = functools.partial(near, 4 * forcing.size <= NEAR_BYTES)
    made = functools.partial(block, 4 * forcing.size <= NEAR_BYTES)
    ends = np.rint(np.cumsum((0,) + SHARES) / sum(SHARES) * share_x).astype(int)
    chunks = tuple(int(n) for n in np.diff(ends) if n > 0)

    tables = {n: transform_table(n) for n in {size_x, size_y, size_z}}
    table_x = [jnp.asarray(t.astype(np.float32).reshape(outer, inner, share_x, size_x)) for t in tables[size_x]]
    table_y = [jnp.asarray(t) for t in tables[size_y]]
    table_z = [jnp.asarray(t) for t in tables[size_z]]

    field = jnp.transpose(forcing, (0, 2, 3, 1))
    cost_x = (2 * field.size * outer * share_x * 3, 8 * field.size)
    spans, start = [], 0
    for count in chunks:
        spans.append((start // 8 * 8, min(-(-(start + count) // 8) * 8, share_x), start, count))
        start += count
    sends = [made((2 * outer * (last - first), 2 * size_x), BF16) for first, last, _, _ in spans]
    sends += [made((count * lines, lanes)) for count in chunks for _ in range(outer)]
    own = call(functools.partial(x_kernel, inner, outer, spans), tuple(sends), cost_x)(field, *table_x)
    ready_x, own = own[: len(chunks)], own[len(chunks) :]
    buffers = [own[c * outer : (c + 1) * outer] for c in range(len(chunks))]
    for k in range(1, inner):
        pairs = [(j, j // inner * inner + partner_int(j % inner, k, inner)) for j in range(north)]
        taken = hold(lax.ppermute(field, "north", pairs))
        for c, (first, last, start, count) in enumerate(spans):
            together = buffers[c] if c == 0 else ()
            other = call(
                functools.partial(other_kernel, outer, count, start - first),
                tuple(made((count * (k + 1 if together else 1) * lines, lanes)) for _ in range(outer)),
                (cost_x[0] * count // share_x, cost_x[1]),
            )(taken, hold(ready_x[c]), *map(hold, together))
            if not together:
                other = call(
                    functools.partial(join_kernel, count, outer),
                    tuple(made((count * (k + 1) * lines, lanes)) for _ in range(outer)),
                    (1000, 16 * outer * count * lines * lanes),
                )(*map(hold, buffers[c]), *map(hold, other))
            buffers[c] = other

    received = []
    for c, count in enumerate(chunks):
        north_order = sorted(range(1, outer), key=NORTH_KEY[min(c, 1)])
        parts = list(buffers[c])
        for s in north_order:
            pairs = [(j, partner_int(j // inner, s, outer) * inner + j % inner) for j in range(north)]
            parts[s] = lax.ppermute(parts[s], "north", pairs)
        cost_y = (2 * count * size_y * size_y * lanes * 3, 8 * count * size_y * lanes)
        blocks = call(
            functools.partial(y_kernel, inner, outer, deep, north_order),
            tuple(made((count, share_y, lanes)) for _ in range(deep)),
            cost_y,
            scratch=(VMEM((2 * size_y, count * lanes), BF16),),
        )(*[hold(parts[s]) for s in (0, *north_order)], *map(hold, table_y))
        sends_z = deep_sends(deep, c)
        steps_z = (0,) + tuple(s for s, _ in sends_z)
        gathered = [blocks[0]] + [lax.ppermute(blocks[s], "deep", pairs) for s, pairs in sends_z]
        received.append((steps_z, gathered, blocks))

    symbol_x, symbol_y, symbol_z, _ = lax.optimization_barrier((symbol_x, symbol_y, symbol_z, received[-1][2]))
    part_x = lax.dynamic_slice_in_dim(symbol_x, lax.axis_index("north") * share_x, share_x)
    part_y = lax.dynamic_slice_in_dim(symbol_y, lax.axis_index("deep") * share_y, share_y)
    symbol = part_x[:, None, None] + part_y[None, :, None] + symbol_z[None, None, :]
    factor = (1.0 - 0.2 * symbol) / (1.0 + 0.2 * symbol)

    result, start = (), 0
    for c, (count, (steps_z, gathered, _)) in enumerate(zip(chunks, received)):
        shape = (fields, share_x, share_y, size_z)
        cost_z = (2 * count * share_y * size_z * size_z * fields * 3, 8 * count * share_y * size_z * fields)
        whole = pl.BlockSpec(memory_space=VMEM)
        anywhere = pl.BlockSpec(memory_space=pl.ANY)
        result = (
            call(
                functools.partial(z_kernel, fields, steps_z, deep, start),
                jax.ShapeDtypeStruct(shape, F32),
                cost_z,
                aliases={len(steps_z) + 3: 0} if c else {},
                scratch=(VMEM((fields, count) + shape[2:], F32), pltpu.SemaphoreType.DMA((fields, CUTS))),
                in_specs=[whole] * (len(steps_z) + 3) + [anywhere] * len(result),
                out_specs=anywhere,
            )(*map(hold, gathered), *map(hold, table_z), hold(factor), *result),
        )
        start += count
    return result[0]


def partner_int(index, step, count):
    return index ^ step if count & (count - 1) == 0 else (index + step) % count


def deep_sends(deep, chunk):
    steps = [(s, [(j, partner_int(j, s, deep)) for j in range(deep)]) for s in range(1, deep)]
    if deep != 4:
        return sorted(steps, key=lambda step: (-step[0].bit_length(), step[0]))
    (one, near), (two, across), (three, ends) = steps
    return [[(three, ends), (two, across), (one, near)], [(two, across), (three, ends), (one, near)]][min(chunk, 1)]


def solution(mesh):
    def step(*arrays):
        return local(mesh.shape["north"], mesh.shape["deep"], *arrays)

    placed = (P(None, None, "north", "deep"), P(), P(), P())
    return jax.shard_map(
        step, mesh=mesh, in_specs=placed, out_specs=P(None, "north", "deep", None), check_vma=False
    )
```

```python
import functools

import jax
import jax.numpy as jnp
import numpy as np
from jax import lax
from jax.experimental import pallas as pl
from jax.experimental.pallas import tpu as pltpu
from jax.sharding import PartitionSpec as P


VMEM = pltpu.VMEM
F32, BF16 = jnp.float32, jnp.bfloat16
SHARES = (6, 10)


def transform_table(count):
    rank = np.arange(count)
    steps = (2 * rank[:, None] + 1) * (2 * rank[None, :] + 1) % (8 * count)
    table = np.cos(np.pi / (4 * count) * steps) * (2.0 / count) ** 0.5
    high = table.astype(np.float32).astype(BF16)
    low = (table - high.astype(np.float64)).astype(np.float32).astype(BF16)
    return high, low


def split(values):
    high = values.astype(BF16)
    return high, (values - high.astype(F32)).astype(BF16)


def dot(a, b, dims):
    return lax.dot_general(a, b, (dims, ((), ())), preferred_element_type=F32)


def dot3(a, b, dims):
    return dot(a[0], b[0], dims) + (dot(a[0], b[1], dims) + dot(a[1], b[0], dims))


CUTS = 2
NORTH_KEY = (lambda s: s, lambda s: s)
NEAR_BYTES = 2**20


def near(fits, array):
    return pltpu.with_memory_space_constraint(array, VMEM) if fits else array


def block(fits, shape, dtype=F32):
    return VMEM(shape, dtype) if fits else jax.ShapeDtypeStruct(shape, dtype)


def partner(index, step, count):
    return index ^ step if count & (count - 1) == 0 else lax.rem(index + step, count)


def source(index, step, count):
    return index ^ step if count & (count - 1) == 0 else lax.rem(index + count - step, count)


def call(kernel, outs, cost, aliases=None, scratch=(), in_specs=None, out_specs=None):
    flops, moved = cost
    kwargs = {}
    if in_specs is not None:
        kwargs["in_specs"] = in_specs
    if out_specs is not None:
        kwargs["out_specs"] = out_specs
    return pl.pallas_call(
        kernel,
        out_shape=outs,
        input_output_aliases=aliases or {},
        scratch_shapes=scratch,
        cost_estimate=pl.CostEstimate(flops=int(flops), bytes_accessed=int(moved), transcendentals=0),
        **kwargs,
    )


def stack_terms(high, low):
    return jnp.concatenate(
        [jnp.concatenate([high, high], 1), jnp.concatenate([low, jnp.zeros_like(low)], 1)], 0
    )


def dot_stacked(stacked, columns, dims):
    rows = stacked.shape[0] // 2
    both = dot(stacked, columns, dims)
    return both[:rows] + both[rows:]


def x_kernel(inner, outer, deep, chunks, *refs):
    field, high, low = refs[:3]
    tables, outs = refs[5 : 5 + len(chunks)], refs[5 + len(chunks) : -1]
    refs[-1][...] = y_table(deep, refs[3:5])
    me = lax.axis_index("north")
    chip, core = me // inner, lax.rem(me, inner)
    shares = [[ref[partner(chip, s, outer), core] for s in range(outer)] for ref in (high, low)]
    table = stack_terms(*(jnp.concatenate(term, 0).astype(BF16) for term in shares))
    for (first, last, _, _), ref in zip(chunks, tables):
        ref[...] = stack_terms(*(jnp.concatenate([rows[first:last] for rows in term], 0).astype(BF16) for term in shares))
    for y, s, value in line_modes(field, table, outer):
        for c, (_, _, start, count) in enumerate(chunks):
            outs[c * outer + s][pl.ds(y, count, stride=field.shape[1]), :] = value[start : start + count]


def line_modes(field, table, outer):
    fields, lines = field.shape[:2]
    rows = table.shape[0] // 2
    share = rows // outer
    pair = 2 if lines % 2 == 0 else 1
    for y in range(0, lines, pair):
        columns = jnp.concatenate([field[f, y + i] for i in range(pair) for f in range(fields)], 0)
        modes = dot_stacked(table, jnp.concatenate(split(columns), 1), ((1,), (1,)))
        lanes = modes.shape[1] // pair
        for i in range(pair):
            for s in range(outer):
                yield y + i, s, modes[s * share : (s + 1) * share, i * lanes : (i + 1) * lanes]


def other_kernel(outer, count, skip, *refs):
    field, table, before, outs = refs[0], refs[1], refs[2:-outer], refs[-outer:]
    lines = field.shape[1]
    done = before[0].shape[0] // (count * lines) if before else 0
    join(count, [before], outs)
    for y, s, value in line_modes(field, table[...], outer):
        outs[s][pl.ds(done * lines + y, count, stride=(done + 1) * lines), :] = value[skip : skip + count]


def join(count, groups, outs):
    total = outs[0].shape[0] // count
    at = 0
    for blocks in groups:
        for block, out in zip(blocks, outs):
            size = block.shape[0] // count
            for r in range(count):
                out[pl.ds(r * total + at, size), :] = block[pl.ds(r * size, size), :]
        at += blocks[0].shape[0] // count if blocks else 0


def join_kernel(count, outer, *refs):
    join(count, (refs[:outer], refs[outer : 2 * outer]), refs[2 * outer :])


def y_table(deep, terms):
    layer, share = lax.axis_index("deep"), terms[0].shape[0] // deep
    return stack_terms(
        *(
            jnp.concatenate([ref[pl.ds(pl.multiple_of(partner(layer, s, deep) * share, share), share), :] for s in range(deep)], 0)
            for ref in terms
        )
    )


def y_kernel(inner, outer, deep, order, *refs):
    parts, table, outs = refs[:outer], refs[outer][...], refs[outer + 1 : outer + 1 + deep]
    terms, total = refs[-1], refs[-1].shape[0] // 2
    me = lax.axis_index("north")
    chip, core = me // inner, lax.rem(me, inner)
    count, share, _ = outs[0].shape
    lines = parts[0].shape[0] // (count * inner)
    lanes = parts[0].shape[1]
    for r in range(count):
        for part, s in zip(parts, (0, *order)):
            for k in range(inner):
                at = (source(chip, s, outer) * inner + source(core, k, inner)) * lines
                at = pl.multiple_of(at, lines)
                for term, value in enumerate(split(part[pl.ds((r * inner + k) * lines, lines), :])):
                    terms[pl.ds(at + term * total, lines), r * lanes : (r + 1) * lanes] = value
    for r in range(0, count, 2):
        group = range(r, min(r + 2, count))
        modes = dot_stacked(table, terms[:, r * lanes : (group[-1] + 1) * lanes], ((1,), (0,)))
        for i in group:
            for s in range(deep):
                outs[s][i] = modes[s * share : (s + 1) * share, (i - r) * lanes : (i - r + 1) * lanes]


def cut_at(count, i):
    return (0, count * 3 // 5, count)[i]


def z_kernel(fields, steps, deep, start, *refs):
    high, low, factor = refs[len(steps) : len(steps) + 3]
    out, stage, sems = refs[-3:]
    order = tuple(dict.fromkeys(steps))
    parts = [[ref for ref, s in zip(refs, steps) if s == step] for step in order]
    layer = lax.axis_index("deep")
    count, modes_y, lanes = refs[0].shape
    depth = lanes // fields
    table = tuple(
        jnp.concatenate([ref[pl.ds(pl.multiple_of(source(layer, s, deep) * depth, depth), depth), :] for s in order], 0)
        for ref in (high, low)
    )
    rows = count * modes_y
    pieces = [split(sum(ref[...] for ref in part).reshape(rows, lanes)) for part in parts]
    copies = []
    for f in range(fields):
        lines = tuple(
            jnp.concatenate([piece[term][:, f * depth : (f + 1) * depth] for piece in pieces], 1) for term in range(2)
        )
        for i in range(CUTS):
            first, last = cut_at(count, i), cut_at(count, i + 1)
            part = tuple(term[first * modes_y : last * modes_y] for term in lines)
            modes = dot3(part, table, ((1,), (0,)))
            stage[f, first:last] = modes.reshape(last - first, modes_y, modes.shape[1]) * factor[start + first : start + last]
            copy = pltpu.make_async_copy(
                stage.at[f, pl.ds(first, last - first)], out.at[f, pl.ds(start + first, last - first)], sems.at[f, i]
            )
            copy.start()
            copies.append(copy)
    for copy in copies:
        copy.wait()


def local(north, deep, forcing, symbol_x, symbol_y, symbol_z):
    fields, size_x, lines, depth = forcing.shape
    size_y, size_z = lines * north, depth * deep
    inner = 2 if north % 2 == 0 else 1
    outer = north // inner
    share_x, share_y = size_x // north, size_y // deep
    lanes = fields * depth
    hold = functools.partial(near, 4 * forcing.size <= NEAR_BYTES)
    made = functools.partial(block, 4 * forcing.size <= NEAR_BYTES)
    ends = np.rint(np.cumsum((0,) + SHARES) / sum(SHARES) * share_x).astype(int)
    chunks = tuple(int(n) for n in np.diff(ends) if n > 0)

    tables = {n: transform_table(n) for n in {size_x, size_y, size_z}}
    table_x = [jnp.asarray(t.astype(np.float32).reshape(outer, inner, share_x, size_x)) for t in tables[size_x]]
    table_y = [jnp.asarray(t) for t in tables[size_y]]
    table_z = [jnp.asarray(t) for t in tables[size_z]]

    field = jnp.transpose(forcing, (0, 2, 3, 1))
    cost_x = (2 * field.size * outer * share_x * 3, 8 * field.size)
    spans, start = [], 0
    for count in chunks:
        spans.append((start // 8 * 8, min(-(-(start + count) // 8) * 8, share_x), start, count))
        start += count
    sends = [made((2 * outer * (last - first), 2 * size_x), BF16) for first, last, _, _ in spans]
    sends += [made((count * lines, lanes)) for count in chunks for _ in range(outer)]
    sends.append(made((2 * size_y, 2 * size_y), BF16))
    *own, ready_y = call(functools.partial(x_kernel, inner, outer, deep, spans), tuple(sends), cost_x)(field, *table_x, *table_y)
    ready_x, own = own[: len(chunks)], own[len(chunks) :]
    buffers = [own[c * outer : (c + 1) * outer] for c in range(len(chunks))]
    for k in range(1, inner):
        pairs = [(j, j // inner * inner + partner_int(j % inner, k, inner)) for j in range(north)]
        taken = hold(lax.ppermute(field, "north", pairs))
        for c, (first, last, start, count) in enumerate(spans):
            together = buffers[c] if c == 0 else ()
            other = call(
                functools.partial(other_kernel, outer, count, start - first),
                tuple(made((count * (k + 1 if together else 1) * lines, lanes)) for _ in range(outer)),
                (cost_x[0] * count // share_x, cost_x[1]),
            )(taken, hold(ready_x[c]), *map(hold, together))
            if not together:
                other = call(
                    functools.partial(join_kernel, count, outer),
                    tuple(made((count * (k + 1) * lines, lanes)) for _ in range(outer)),
                    (1000, 16 * outer * count * lines * lanes),
                )(*map(hold, buffers[c]), *map(hold, other))
            buffers[c] = other

    received = []
    for c, count in enumerate(chunks):
        north_order = sorted(range(1, outer), key=NORTH_KEY[min(c, 1)])
        parts = list(buffers[c])
        for s in north_order:
            pairs = [(j, partner_int(j // inner, s, outer) * inner + j % inner) for j in range(north)]
            parts[s] = lax.ppermute(parts[s], "north", pairs)
        cost_y = (2 * count * size_y * size_y * lanes * 3, 8 * count * size_y * lanes)
        blocks = call(
            functools.partial(y_kernel, inner, outer, deep, north_order),
            tuple(made((count, share_y, lanes)) for _ in range(deep)),
            cost_y,
            scratch=(VMEM((2 * size_y, count * lanes), BF16),),
        )(*[hold(parts[s]) for s in (0, *north_order)], hold(ready_y))
        sends_z = deep_sends(deep, c)
        steps_z = (0,) + tuple(s for s, _ in sends_z)
        gathered = [blocks[0]] + [lax.ppermute(blocks[s], "deep", pairs) for s, pairs in sends_z]
        received.append((steps_z, gathered, blocks))

    symbol_x, symbol_y, symbol_z, _ = lax.optimization_barrier((symbol_x, symbol_y, symbol_z, received[-1][2]))
    part_x = lax.dynamic_slice_in_dim(symbol_x, lax.axis_index("north") * share_x, share_x)
    part_y = lax.dynamic_slice_in_dim(symbol_y, lax.axis_index("deep") * share_y, share_y)
    symbol = part_x[:, None, None] + part_y[None, :, None] + symbol_z[None, None, :]
    factor = (1.0 - 0.2 * symbol) / (1.0 + 0.2 * symbol)

    result, start = (), 0
    for c, (count, (steps_z, gathered, _)) in enumerate(zip(chunks, received)):
        shape = (fields, share_x, share_y, size_z)
        cost_z = (2 * count * share_y * size_z * size_z * fields * 3, 8 * count * share_y * size_z * fields)
        whole = pl.BlockSpec(memory_space=VMEM)
        anywhere = pl.BlockSpec(memory_space=pl.ANY)
        result = (
            call(
                functools.partial(z_kernel, fields, steps_z, deep, start),
                jax.ShapeDtypeStruct(shape, F32),
                cost_z,
                aliases={len(steps_z) + 3: 0} if c else {},
                scratch=(VMEM((fields, count) + shape[2:], F32), pltpu.SemaphoreType.DMA((fields, CUTS))),
                in_specs=[whole] * (len(steps_z) + 3) + [anywhere] * len(result),
                out_specs=anywhere,
            )(*map(hold, gathered), *map(hold, table_z), hold(factor), *result),
        )
        start += count
    return result[0]


def partner_int(index, step, count):
    return index ^ step if count & (count - 1) == 0 else (index + step) % count


def deep_sends(deep, chunk):
    steps = [(s, [(j, partner_int(j, s, deep)) for j in range(deep)]) for s in range(1, deep)]
    if deep != 4:
        return sorted(steps, key=lambda step: (-step[0].bit_length(), step[0]))
    (one, near), (two, across), (three, ends) = steps
    return [[(three, ends), (two, across), (one, near)], [(two, across), (three, ends), (one, near)]][min(chunk, 1)]


def solution(mesh):
    def step(*arrays):
        return local(mesh.shape["north"], mesh.shape["deep"], *arrays)

    placed = (P(None, None, "north", "deep"), P(), P(), P())
    return jax.shard_map(
        step, mesh=mesh, in_specs=placed, out_specs=P(None, "north", "deep", None), check_vma=False
    )
```
